32 devices in a mesh: grp: 4 (over y, core), sub: 8 (over z, x).
Axes of the slice: x: 2, y: 2, z: 4, core: 2. Of those that a mesh axis runs over, the one named last changes fastest.
Arguments:
- fields: float32 [4, 35, 8192], P(None, None, ('grp', 'sub')), may hold values from -6 to 6
- section_store: float32 [4, 35, 8192], P(None, None, ('grp', 'sub')), may hold values from -6 to 6
- metric_terms: float32 [9, 8192], P(None, ('grp', 'sub')), may hold values from -6 to 6
- normals: float32 [4, 3, 8192], P(None, None, ('grp', 'sub')), may hold values from -3 to 3
- face_scale: float32 [4, 8192], P(None, ('grp', 'sub')), may hold values from 1 to 4
- damping: float32 [8192], P(('grp', 'sub')), may hold values from 1 to 10
- absorb_mask: int32 [8192], P(('grp', 'sub')), may hold values from 0 to 1
- refine_level: int32 [8192], P(('grp', 'sub')), may hold values from 0 to 2
- face_source: int32 [4, 8192], P(None, ('grp', 'sub')), may hold values from -1 to 1343, as said below
- orientation: int32 [4, 8192], P(None, ('grp', 'sub')), may hold values from 0 to 5, as said below
- derivative: float32 [3, 35, 35], replicated, may hold values from -1 to 1
- lift_matrix: float32 [35, 60], replicated, may hold values from -0.75 to 0.75
Outputs:
- fields_next: float32 [4, 35, 8192], P(None, None, ('grp', 'sub'))
- store_next: float32 [4, 35, 8192], P(None, None, ('grp', 'sub'))
- absorbed_energy: float32 [], replicated
The draws below stay inside these ranges and needn't reach their ends.
Inputs may be any that keep to these rules, and one draw needn't show every extreme that they name: `face_source`: the neighbour relation is symmetric: the neighbour of a face's neighbour is the face itself, every code at or above 1024 names a slot used by exactly one face of its device, and a face's neighbour on device d holds the matching slot as in the reference program. A device uses the slots of a block from rank 0 on without gaps; it never uses block s (its own sub index), nor block 8 at the first grp index or block 9 at the last. For a sub peer b with |b - s| <= 4 at most 32 ranks are used, for other peers at most 8, and across grp at most 32; in every draw some near pair uses all 32, some farther pair all 8, and some pair across grp all 32. Local neighbours lie on the same device. `orientation`: paired faces have inverse orientations: 1 and 2 swap, 0, 3, 4 and 5 stay.
All inputs are finite; a program needn't handle non-finite values.
Results may differ from the reference program's by a relative error of at most 0.0003.
Values sent between devices are 32-bit elements; how exact they have to be, the bound alone decides.
A program may use at most 64 MiB of HBM per device.

```python
import math
import jax
import jax.numpy as jnp
import numpy as np
from jax import lax

VOLUME_NODES = 35
FACE_NODES = 15
NEAR_PEERS = 4
LOCAL_ELEMENTS = 256
PEER_SLOTS = 32
ELEMENTS = 8192
N_GRP = 4
N_SUB = 8


def link_tables(key):
    devices = N_GRP * N_SUB
    per_device = LOCAL_ELEMENTS
    slot_width = PEER_SLOTS
    narrow = slot_width // 4
    block_total = N_SUB + 2
    box_size = block_total * slot_width
    face_total = 4 * per_device
    subkeys = jax.random.split(jax.random.fold_in(key, 7301), 10)
    member_ids = jnp.arange(N_SUB, dtype=jnp.int32)
    spread = jnp.abs(member_ids[:, None] - member_ids[None, :])
    near_draw = jax.random.randint(subkeys[0], (N_GRP, N_SUB, N_SUB), slot_width // 2, slot_width + 1)
    far_draw = jax.random.randint(subkeys[1], (N_GRP, N_SUB, N_SUB), 0, narrow + 1)
    upper_part = jnp.triu(jnp.where(spread[None] <= NEAR_PEERS, near_draw, far_draw), 1)
    counts = upper_part + jnp.transpose(upper_part, (0, 2, 1))
    start_at = jax.random.randint(subkeys[2], (N_GRP,), 0, N_SUB - NEAR_PEERS - 1)
    group_ids = jnp.arange(N_GRP, dtype=jnp.int32)
    counts = counts.at[group_ids, start_at, start_at + 1].set(slot_width)
    counts = counts.at[group_ids, start_at + 1, start_at].set(slot_width)
    counts = counts.at[group_ids, start_at, start_at + NEAR_PEERS + 1].set(narrow)
    counts = counts.at[group_ids, start_at + NEAR_PEERS + 1, start_at].set(narrow)
    slab_counts = jax.random.randint(subkeys[3], (N_GRP - 1, N_SUB), slot_width // 2, slot_width + 1)
    slab_group = jax.random.randint(subkeys[4], (), 0, N_GRP - 1)
    slab_member = jax.random.randint(subkeys[5], (), 0, N_SUB)
    slab_counts = slab_counts.at[slab_group, slab_member].set(slot_width)
    zero_row = jnp.zeros((1, N_SUB), jnp.int32)
    down_counts = jnp.concatenate([zero_row, slab_counts], 0).reshape(devices)
    upward = jnp.concatenate([slab_counts, zero_row], 0).reshape(devices)
    block_counts = jnp.concatenate([counts.reshape(devices, N_SUB), down_counts[:, None], upward[:, None]], 1)
    block_ends = jnp.cumsum(block_counts, 1)
    begins = block_ends - block_counts
    remote_total = block_ends[:, -1]
    leftover = face_total - remote_total
    wall_draw = jax.random.randint(subkeys[6], (devices,), 0, 1 << 20)
    wall_count = leftover % 2 + 2 * (wall_draw % (leftover // 16 + 1))
    pair_start = remote_total + wall_count
    position = jnp.arange(face_total, dtype=jnp.int32)
    block_index = jax.vmap(lambda row: jnp.searchsorted(row, position, side='right'))(block_ends).astype(jnp.int32)
    block_index = jnp.minimum(block_index, block_total - 1)
    rank = position[None, :] - jnp.take_along_axis(begins, block_index, 1)
    is_remote = position[None, :] < remote_total[:, None]
    is_pair = position[None, :] >= pair_start[:, None]
    offset_pair = position[None, :] - pair_start[:, None]
    partner_pos = jnp.clip(pair_start[:, None] + jnp.bitwise_xor(offset_pair, 1), 0, face_total - 1)
    orders = jax.vmap(lambda sub_key: jax.random.permutation(sub_key, face_total))(jax.random.split(subkeys[7], devices)).astype(jnp.int32)
    partner_face = jnp.take_along_axis(orders, partner_pos, 1)
    code_pos = jnp.where(is_remote, face_total + block_index * slot_width + rank, jnp.where(is_pair, partner_face, -1))
    inverse = jnp.array([0, 2, 1, 3, 4, 5], jnp.int32)
    own_turn = jax.random.randint(subkeys[8], (devices, face_total), 0, 6)
    pair_lead = offset_pair % 2 == 0
    local_turn = jnp.where(pair_lead, own_turn, inverse[jnp.take_along_axis(own_turn, partner_pos, 1)])
    link_turn = jax.random.randint(subkeys[9], (devices * box_size,), 0, 6)
    device = jnp.arange(devices, dtype=jnp.int32)[:, None]
    group_index = device // N_SUB
    member = device % N_SUB
    peer_dev = jnp.where(block_index < N_SUB, group_index * N_SUB + block_index, jnp.where(block_index == N_SUB, device - N_SUB, device + N_SUB))
    peer_slot = jnp.where(block_index < N_SUB, member * slot_width + rank, jnp.where(block_index == N_SUB, (N_SUB + 1) * slot_width + rank, N_SUB * slot_width + rank))
    own_slot = block_index * slot_width + rank
    mine = link_turn[jnp.clip(device * box_size + own_slot, 0, devices * box_size - 1)]
    theirs = inverse[link_turn[jnp.clip(peer_dev * box_size + peer_slot, 0, devices * box_size - 1)]]
    remote_turn = jnp.where(device < peer_dev, mine, theirs)
    turn_pos = jnp.where(is_remote, remote_turn, jnp.where(is_pair, local_turn, own_turn))
    device_rows = jnp.broadcast_to(device, (devices, face_total))
    source_faces = jnp.zeros((devices, face_total), jnp.int32).at[device_rows, orders].set(code_pos)
    turn_faces = jnp.zeros((devices, face_total), jnp.int32).at[device_rows, orders].set(turn_pos)
    source_out = jnp.transpose(source_faces.reshape(devices, 4, per_device), (1, 0, 2)).reshape(4, devices * per_device)
    turn_out = jnp.transpose(turn_faces.reshape(devices, 4, per_device), (1, 0, 2)).reshape(4, devices * per_device)
    return (source_out, turn_out)


def draw_face_source(key, part):
    return link_tables(key)[0]


def draw_orientation(key, part):
    return link_tables(key)[1]


def draw_absorb_mask(key, part):
    total_elements = LOCAL_ELEMENTS * N_GRP * N_SUB
    element = jnp.arange(total_elements, dtype=jnp.int32)
    limit = 150 + 300 * element // total_elements
    picks = jax.random.randint(jax.random.fold_in(key, 4409), (total_elements,), 0, 1000)
    return (picks < limit).astype(jnp.int32)


def plant(result, rng, least, high):
    extent = result.shape
    place = [jax.random.randint(jax.random.fold_in(rng, axis), (), 0, extent[axis]) for axis in range(len(extent))]
    result = result.at[tuple(place)].set(least)
    longest = extent.index(max(extent))
    place[longest] = (place[longest] + 1) % extent[longest]
    return result.at[tuple(place)].set(high)


def block_scale(key, dims, shards, smallest, high):
    loudness, own = 1.0, jax.random.fold_in(key, 6)
    for axis_at, parts in shards:
        heights = jnp.exp(jax.random.uniform(jax.random.fold_in(own, axis_at), (parts,), jnp.float32, smallest / len(shards), high / len(shards)))
        loudness = loudness * jnp.repeat(heights, dims[axis_at] // parts).reshape([-1 if axis == axis_at else 1 for axis in range(len(dims))])
    return loudness


def centred(key, extent, scale, reach, shards=(), kind=jnp.bfloat16):
    values = jax.random.normal(key, extent, jnp.float32) * scale
    if len(shards) > 0:
        values = block_scale(key, extent, shards, -0.22, 0.18) * values
    return jnp.clip(values, min=-reach, max=reach).astype(kind)


def setup_inputs(seed: int = 0) -> dict:
    key_list = jax.random.split(jax.random.key(seed), 13)
    fields = centred(key_list[0], (4, VOLUME_NODES, ELEMENTS), 1.0, 6.0, ((2, 32),), jnp.float32)
    section_store = centred(key_list[1], (4, VOLUME_NODES, ELEMENTS), 1.0, 6.0, ((2, 32),), jnp.float32)
    metric_terms = centred(key_list[2], (9, ELEMENTS), 1.0, 6.0, ((1, 32),), jnp.float32)
    normals = centred(key_list[3], (4, 3, ELEMENTS), 0.577, 3.0, ((2, 32),), jnp.float32)
    face_scale = jnp.clip(jnp.exp(math.log(4.0) - 1.3862944 * jax.random.uniform(key_list[4], (4, ELEMENTS), jnp.float32) ** block_scale(key_list[4], (4, ELEMENTS), ((1, 32),), -0.2, 0.2)), 1.0, 4.0)
    damping = jnp.clip(jnp.exp(math.log(10.0) - 2.3025851 * jax.random.uniform(key_list[5], (ELEMENTS,), jnp.float32) ** block_scale(key_list[5], (ELEMENTS,), ((0, 32),), -0.2, 0.2)), 1.0, 10.0)
    absorb_mask = draw_absorb_mask(jax.random.fold_in(key_list[12], 71), 0)
    refine_level = plant(jax.random.randint(key_list[7], (ELEMENTS,), 0, 3), jax.random.fold_in(key_list[7], 1), 0, 2).astype(jnp.int32)
    face_source = draw_face_source(jax.random.fold_in(key_list[12], 71), 0)
    orientation = draw_orientation(jax.random.fold_in(key_list[12], 71), 0)
    derivative = centred(key_list[10], (3, VOLUME_NODES, VOLUME_NODES), VOLUME_NODES ** -0.5, 1.0, (), jnp.float32)
    lift_matrix = centred(key_list[11], (VOLUME_NODES, 4 * FACE_NODES), (4 * FACE_NODES) ** -0.5, 0.75, (), jnp.float32)
    return dict(fields=fields, section_store=section_store, metric_terms=metric_terms, normals=normals, face_scale=face_scale, damping=damping, absorb_mask=absorb_mask, refine_level=refine_level, face_source=face_source, orientation=orientation, derivative=derivative, lift_matrix=lift_matrix)


RUNGE_CARRY = -567301805773.0 / 1357537059087.0
RUNGE_ADVANCE = 5161836677717.0 / 13612068292357.0
TIME_STEP = 0.02


def node_tables():
    volume_list = [(first_part, second_part, third_part, 4 - first_part - second_part - third_part)
                   for first_part in range(5) for second_part in range(5 - first_part)
                   for third_part in range(5 - first_part - second_part)]
    triples = [(first_part, second_part, 4 - first_part - second_part)
               for first_part in range(5) for second_part in range(5 - first_part)]
    face_index = np.zeros((4, 15), np.int32)
    for facet in range(4):
        others = [corner for corner in range(4) if corner != facet]
        for node_pos in range(15):
            corners = [0, 0, 0, 0]
            for place_pos in range(3):
                corners[others[place_pos]] = triples[node_pos][place_pos]
            face_index[facet, node_pos] = volume_list.index(tuple(corners))
    vertex_orders = [(0, 1, 2), (1, 2, 0), (2, 0, 1), (0, 2, 1), (2, 1, 0), (1, 0, 2)]
    turn_index = np.zeros((6, 15), np.int32)
    for option in range(6):
        vertex_order = vertex_orders[option]
        for node_pos in range(15):
            triple = triples[node_pos]
            turned = (triple[vertex_order[0]], triple[vertex_order[1]], triple[vertex_order[2]])
            turn_index[option, node_pos] = triples.index(turned)
    return face_index, turn_index


def turn_matrices():
    face_index, turn_index = node_tables()
    table = np.zeros((6, 15, 15), np.float32)
    for option in range(6):
        for node_pos in range(15):
            table[option, node_pos, turn_index[option, node_pos]] = 1.0
    return jnp.asarray(table, jnp.float32)


def advance(fields, section_store, metric_terms, normals, face_scale, damping, absorb_mask, refine_level,
            face_codes, orient_flat, inner_cols, outer_cols, derivative, lift_matrix):
    elements_here = fields.shape[2]
    total_faces = 4 * elements_here
    turning = turn_matrices()
    inside = inner_cols.reshape(4, FACE_NODES, total_faces)
    gathered = outer_cols.reshape(4, FACE_NODES, total_faces)
    outside = gathered
    for option in range(1, 6):
        turned = jnp.einsum("jk,ckx->cjx", turning[option], gathered, precision=lax.Precision.HIGHEST)
        outside = jnp.where(orient_flat[None, None, :] == option, turned, outside)
    normal_flat = jnp.transpose(normals, (1, 0, 2)).reshape(3, total_faces)
    on_wall = (face_codes < 0)[None, :]
    press_in = inside[0]
    veloc_in = inside[1:]
    normal_in = jnp.sum(normal_flat[:, None, :] * veloc_in, 0)
    press_out = jnp.where(on_wall, press_in, outside[0])
    veloc_out = jnp.where(on_wall[None], veloc_in - 2.0 * normal_flat[:, None, :] * normal_in[None], outside[1:])
    press_jump = press_in - press_out
    normal_jump = jnp.sum(normal_flat[:, None, :] * (veloc_in - veloc_out), 0)
    growth = jnp.exp2(refine_level.astype(jnp.float32))
    weight_face = (face_scale * growth[None, :]).reshape(total_faces)
    flux_press = 0.5 * weight_face[None, :] * (normal_jump - press_jump)
    flux_veloc = 0.5 * weight_face[None, None, :] * normal_flat[:, None, :] * (press_jump - normal_jump)[None]
    flux_all = jnp.concatenate([flux_press[None], flux_veloc], 0).reshape(4, FACE_NODES, 4, elements_here)
    lifted = jnp.einsum("nfj,cjfe->cne", lift_matrix.reshape(VOLUME_NODES, 4, FACE_NODES), flux_all,
                        precision=lax.Precision.HIGHEST)
    slopes = jnp.einsum("dnm,cme->dcne", derivative, fields, precision=lax.Precision.HIGHEST)
    metric = metric_terms.reshape(3, 3, elements_here) * growth[None, None, :]
    physical = jnp.einsum("ide,dcne->icne", metric, slopes, precision=lax.Precision.HIGHEST)
    absorb = damping * absorb_mask.astype(jnp.float32)
    diverge = physical[0, 1] + physical[1, 2] + physical[2, 3]
    volume = jnp.concatenate([-diverge[None], -physical[:, 0]], 0)
    change = volume + lifted - absorb[None, None, :] * fields
    store_next = RUNGE_CARRY * section_store + TIME_STEP * change
    fields_next = fields + RUNGE_ADVANCE * store_next
    energy = jnp.sum(absorb * jnp.sum(fields_next * fields_next, (0, 1)))
    return fields_next, store_next, energy


def reference(fields, section_store, metric_terms, normals, face_scale, damping, absorb_mask, refine_level,
              face_source, orientation, derivative, lift_matrix):
    face_index, turn_index = node_tables()
    devices = N_GRP * N_SUB
    per_device = LOCAL_ELEMENTS
    slot_width = PEER_SLOTS
    box_size = (N_SUB + 2) * slot_width
    traces = fields[:, face_index, :]
    own_cols = jnp.transpose(traces.reshape(4, 4, FACE_NODES, devices, per_device), (0, 2, 3, 1, 4))
    own_cols = own_cols.reshape(4 * FACE_NODES, 4 * ELEMENTS)
    element = jnp.arange(ELEMENTS, dtype=jnp.int32)
    device = jnp.broadcast_to((element // per_device)[None, :], (4, ELEMENTS))
    within = jnp.broadcast_to((element % per_device)[None, :], (4, ELEMENTS))
    facet = jnp.arange(4, dtype=jnp.int32)[:, None]
    column = device * (4 * per_device) + facet * per_device + within
    face_codes = face_source
    is_local = (face_codes >= 0) & (face_codes < 4 * per_device)
    is_remote = face_codes >= 4 * per_device
    local_col = device * (4 * per_device) + jnp.clip(face_codes, 0, 4 * per_device - 1)
    slot_index = jnp.where(is_remote, face_codes - 4 * per_device, 0)
    block_index = slot_index // slot_width
    rank = slot_index % slot_width
    group_index = device // N_SUB
    member = device % N_SUB
    peer_dev = jnp.where(block_index < N_SUB, group_index * N_SUB + block_index,
                         jnp.where(block_index == N_SUB, device - N_SUB, device + N_SUB))
    peer_slot = jnp.where(block_index < N_SUB, member * slot_width + rank,
                          jnp.where(block_index == N_SUB, (N_SUB + 1) * slot_width + rank, N_SUB * slot_width + rank))
    owner_place = jnp.where(is_remote, device * box_size + slot_index, devices * box_size).astype(jnp.int32)
    slot_owner = jnp.zeros((devices * box_size,), jnp.int32).at[owner_place.reshape(-1)].set(
        column.reshape(-1), mode="drop")
    remote_col = slot_owner[jnp.clip(peer_dev * box_size + peer_slot, 0, devices * box_size - 1).astype(jnp.int32)]
    partner = jnp.where(is_local, local_col, jnp.where(is_remote, remote_col, 0)).astype(jnp.int32)

    def by_device(array):
        return jnp.transpose(array.reshape(array.shape[:-1] + (devices, per_device)),
                             (array.ndim - 1,) + tuple(range(array.ndim - 1)) + (array.ndim,))

    fields_d = by_device(fields)
    store_d = by_device(section_store)
    metric_d = by_device(metric_terms)
    normals_d = by_device(normals)
    scale_d = by_device(face_scale)
    damping_d = damping.reshape(devices, per_device)
    mask_d = absorb_mask.reshape(devices, per_device)
    level_d = refine_level.reshape(devices, per_device)
    codes_d = by_device(face_source).reshape(devices, 4 * per_device)
    orient_d = by_device(orientation).reshape(devices, 4 * per_device)
    partner_d = by_device(partner).reshape(devices, 4 * per_device)
    inner_d = jnp.transpose(own_cols.reshape(4 * FACE_NODES, devices, 4 * per_device), (1, 0, 2))

    def one_device(pieces):
        (fields_p, store_p, metric_p, normals_p, scale_p, damping_p, mask_p, level_p,
         codes_p, orient_p, inner_p, partner_p) = pieces
        outer_p = jnp.take(own_cols, partner_p, axis=1)
        return advance(fields_p, store_p, metric_p, normals_p, scale_p, damping_p, mask_p, level_p,
                       codes_p, orient_p, inner_p, outer_p, derivative, lift_matrix)

    fields_out, store_out, energies = lax.map(one_device, (fields_d, store_d, metric_d, normals_d, scale_d,
                                                          damping_d, mask_d, level_d, codes_d, orient_d,
                                                          inner_d, partner_d))
    fields_next = jnp.transpose(fields_out, (1, 2, 0, 3)).reshape(4, VOLUME_NODES, ELEMENTS)
    store_next = jnp.transpose(store_out, (1, 2, 0, 3)).reshape(4, VOLUME_NODES, ELEMENTS)
    absorbed_energy = jnp.sum(energies) / (ELEMENTS * VOLUME_NODES)
    return (fields_next, store_next, absorbed_energy)
```

```python
import functools

import jax
import jax.numpy as jnp
import numpy as np
from jax import lax
from jax.experimental import pallas as pl
from jax.experimental.pallas import tpu as pltpu
from jax.sharding import PartitionSpec as P

VOLUME_NODES = 35
FACE_NODES = 15
NEAR_PEERS = 4
NODE_PAD = 48
SLOPE_PAD = 40
ROWS = 64

RUNGE_CARRY = -567301805773.0 / 1357537059087.0
RUNGE_ADVANCE = 5161836677717.0 / 13612068292357.0
TIME_STEP = 0.02
OPERANDS = 13
MESH = pl.DeviceIdType.MESH


def node_tables():
    volume_list = [
        (a, b, c, 4 - a - b - c) for a in range(5) for b in range(5 - a) for c in range(5 - a - b)
    ]
    triples = [(a, b, 4 - a - b) for a in range(5) for b in range(5 - a)]
    face_index = np.zeros((4, 15), np.int32)
    for facet in range(4):
        others = [corner for corner in range(4) if corner != facet]
        for node_pos in range(15):
            corners = [0, 0, 0, 0]
            for place_pos in range(3):
                corners[others[place_pos]] = triples[node_pos][place_pos]
            face_index[facet, node_pos] = volume_list.index(tuple(corners))
    vertex_orders = [(0, 1, 2), (1, 2, 0), (2, 0, 1), (0, 2, 1), (2, 1, 0), (1, 0, 2)]
    turn_index = np.zeros((6, 15), np.int32)
    for option in range(6):
        q = vertex_orders[option]
        for node_pos in range(15):
            t = triples[node_pos]
            turn_index[option, node_pos] = triples.index((t[q[0]], t[q[1]], t[q[2]]))
    return face_index, turn_index


def constant_table():
    face_index, turn_index = node_tables()
    table = np.zeros((ROWS, 1024), np.float32)
    for f in range(4):
        for j in range(15):
            table[f * 16 + j, face_index[f, j]] = 1.0
            table[f * 15 + j, 896 + f * 16 + j] = 1.0
    for part in range(2):
        for o in range(6):
            for c in range(4):
                for j in range(15):
                    col = 128 + part * 384 + o * 64 + c * 16 + turn_index[o, j]
                    table[c * 16 + j, col] = 1.0
    return jnp.asarray(table, jnp.bfloat16)


def split(value):
    high = value.astype(jnp.bfloat16)
    low = (value - high.astype(jnp.float32)).astype(jnp.bfloat16)
    return high, low


def dot(left, right):
    return jnp.dot(left, right, preferred_element_type=jnp.float32)


def dot3(left, right):
    (lh, ll), (rh, rl) = left, right
    return dot(lh, rh) + (dot(lh, rl) + dot(ll, rh))


def flat_row(ref_rows):
    return jnp.concatenate(ref_rows, axis=1)


def kernel(
    n_grp,
    n_sub,
    direct,
    *refs,
):
    operands, rest = refs[:OPERANDS], refs[OPERANDS:]
    results, rest = rest[:4], rest[4:]
    copies, rest = results[:2] + rest[: OPERANDS - 2], rest[OPERANDS - 2 :]
    body(n_grp, n_sub, direct, operands, *copies, *results[2:], *rest)


def body(
    n_grp,
    n_sub,
    direct,
    operands,
    fields,
    store,
    metric,
    normals,
    face_scale,
    damping,
    mask,
    level,
    source,
    orient,
    derivative,
    lift,
    table,
    change_out,
    energy_out,
    fpad,
    dpad,
    lpad,
    outbox,
    inbox,
    base,
    energy_row,
    energy_mid,
    energy_a,
    energy_b,
    send_sem,
    recv_sem,
    esend_a,
    erecv_a,
    esend_b,
    erecv_b,
    load_sem,
):
    copies = (
        fields,
        store,
        metric,
        normals,
        face_scale,
        damping,
        mask,
        level,
        source,
        orient,
        derivative,
        lift,
        table,
    )
    loads = [
        pltpu.make_async_copy(operands[i], copies[i], load_sem.at[i]) for i in range(OPERANDS)
    ]
    early = (0, 8, 12)
    elements = face_scale.shape[1]
    tiles = elements // 128
    faces = 4 * elements
    half = elements // 16
    n_blocks = n_sub + 2

    def node_rows(c, t):
        return pl.ds(t * 4 + c, VOLUME_NODES, stride=4 * tiles)

    def read(ref, c):
        return jnp.concatenate([ref[node_rows(c, t), :] for t in range(tiles)], axis=1)

    def write(ref, c, value):
        for t in range(tiles):
            ref[node_rows(c, t), :] = value[:, t * 128 : (t + 1) * 128]

    g = lax.axis_index("grp")
    s = lax.axis_index("sub")

    def sub_peer(k):
        return lax.rem(s + k, n_sub)

    def grp_peer(k):
        return lax.rem(g + k, n_grp)

    inbox[...] = jnp.zeros_like(inbox)
    for i in early:
        loads[i].start()
    for i in range(OPERANDS):
        if i not in early:
            loads[i].start()
    barrier = pltpu.get_barrier_semaphore()
    greeted = 0
    for kg in range(n_grp):
        for ks in range(n_sub):
            if (kg, ks) == (0, 0) or not (direct or kg == 0 or ks == 0):
                continue
            pl.semaphore_signal(
                barrier, inc=1, device_id=(grp_peer(kg), sub_peer(ks)), device_id_type=MESH
            )
            greeted += 1
    for i in early:
        loads[i].wait()

    fpad[VOLUME_NODES:, :] = jnp.zeros((NODE_PAD - VOLUME_NODES, faces), jnp.float32)
    for c in range(4):
        fpad[0:VOLUME_NODES, c * elements : (c + 1) * elements] = read(fields, c)
    field_parts = split(fpad[...])
    pick = table[:, 0:NODE_PAD]

    def by_face(value):
        return jnp.concatenate(
            [
                jnp.concatenate(
                    [
                        value[f * 16 : (f + 1) * 16, c * elements : (c + 1) * elements]
                        for c in range(4)
                    ],
                    axis=0,
                )
                for f in range(4)
            ],
            axis=1,
        )

    inner_high = by_face(dot(pick, field_parts[0]))
    inner_low = by_face(dot(pick, field_parts[1]))
    codes = flat_row([source[f : f + 1, :] for f in range(4)])
    high_b = inner_high.astype(jnp.bfloat16)
    low_b = inner_low.astype(jnp.bfloat16)

    def slots_hot(part):
        row = lax.broadcasted_iota(jnp.int32, (n_blocks * half, faces), 0)
        slot = (row // half) * (2 * half) + part * half + row % half
        return jnp.where(slot == codes - faces, 1.0, 0.0).astype(jnp.bfloat16)

    hot = [slots_hot(0), slots_hot(1)]
    nothing = jnp.zeros_like(high_b)
    packed = None
    for part in range(2):
        for value in (high_b, low_b):
            weights = jnp.concatenate([value, nothing] if part == 0 else [nothing, value], axis=0)
            term = lax.dot_general(
                hot[part], weights, (((1,), (1,)), ((), ())), preferred_element_type=jnp.float32
            )
            packed = term if packed is None else packed + term
    outbox[...] = packed.reshape(n_blocks, half, 2 * ROWS)

    pl.semaphore_wait(barrier, greeted)

    def sub_copy(k, rows):
        peer = sub_peer(k)
        return pltpu.make_async_remote_copy(
            src_ref=outbox.at[peer, pl.ds(0, rows)],
            dst_ref=inbox.at[s, pl.ds(0, rows)],
            send_sem=send_sem.at[peer],
            recv_sem=recv_sem.at[s],
            device_id=(g, peer),
            device_id_type=MESH,
        )

    def sub_arrival(k, rows):
        peer = sub_peer(k)
        return pltpu.make_async_remote_copy(
            src_ref=outbox.at[peer, pl.ds(0, rows)],
            dst_ref=inbox.at[peer, pl.ds(0, rows)],
            send_sem=send_sem.at[peer],
            recv_sem=recv_sem.at[peer],
            device_id=(g, peer),
            device_id_type=MESH,
        )

    def grp_copy(up):
        block, landing = (n_sub + 1, n_sub) if up else (n_sub, n_sub + 1)
        peer = jnp.minimum(g + 1, n_grp - 1) if up else jnp.maximum(g - 1, 0)
        return pltpu.make_async_remote_copy(
            src_ref=outbox.at[block],
            dst_ref=inbox.at[landing],
            send_sem=send_sem.at[block],
            recv_sem=recv_sem.at[landing],
            device_id=(peer, s),
            device_id_type=MESH,
        )

    def each_sub(make, act):
        for k in range(1, n_sub):
            gap = jnp.abs(sub_peer(k) - s)

            @pl.when(gap <= NEAR_PEERS)
            def _():
                act(make(k, half))

            @pl.when(gap > NEAR_PEERS)
            def _():
                act(make(k, half // 2))

    each_sub(sub_copy, lambda copy: copy.start())

    @pl.when(g > 0)
    def _():
        grp_copy(False).start()

    @pl.when(g < n_grp - 1)
    def _():
        grp_copy(True).start()

    for i in range(OPERANDS):
        if i not in early:
            loads[i].wait()
    growth = jnp.exp2(level[...].astype(jnp.float32))
    absorb = damping[...] * mask[...].astype(jnp.float32)
    dpad[...] = jnp.zeros_like(dpad)
    for d in range(3):
        dpad[d * SLOPE_PAD : d * SLOPE_PAD + VOLUME_NODES, 0:VOLUME_NODES] = derivative[d]
    slopes = dot3(split(dpad[...]), field_parts)

    def slope(d, c):
        return slopes[
            d * SLOPE_PAD : (d + 1) * SLOPE_PAD, c * elements : (c + 1) * elements
        ]

    def field(c):
        return fpad[0:VOLUME_NODES, c * elements : (c + 1) * elements]

    scaled = metric[...] * growth
    for c in range(4):
        total = None
        for x in range(3) if c == 0 else (c - 1,):
            for y in range(3):
                term = scaled[3 * x + y : 3 * x + y + 1, :] * slope(y, x + 1 if c == 0 else 0)
                total = term if total is None else total + term
        change = -total[0:VOLUME_NODES] - absorb * field(c)
        base[c, 0:VOLUME_NODES, :] = change

    lpad[...] = jnp.zeros_like(lpad)
    lpad[0:VOLUME_NODES, 0:60] = lift[...]
    spread = table[:, 896:960]
    lift_parts = tuple(dot(part, spread).astype(jnp.bfloat16) for part in split(lpad[...]))

    stacked = jnp.concatenate([high_b, low_b], axis=0)
    gathered = None
    for f in range(4):
        row = lax.broadcasted_iota(jnp.int32, (elements, faces), 0) + f * elements
        chosen = jnp.where(row == codes, 1.0, 0.0).astype(jnp.bfloat16)
        term = dot(stacked[:, f * elements : (f + 1) * elements], chosen)
        gathered = term if gathered is None else gathered + term

    each_sub(sub_arrival, lambda copy: copy.wait_recv())

    @pl.when(g > 0)
    def _():
        grp_copy(True).wait_recv()

    @pl.when(g < n_grp - 1)
    def _():
        grp_copy(False).wait_recv()

    arrived = inbox[...].reshape(n_blocks * half, 2 * ROWS).T
    for part in range(2):
        pieces = split(arrived[part * ROWS : (part + 1) * ROWS])
        gathered = gathered + dot(jnp.concatenate(pieces, axis=0), hot[part])

    turns = flat_row([orient[f : f + 1, :] for f in range(4)])
    pieces = []
    for part in range(2):
        value = gathered[part * ROWS : (part + 1) * ROWS]
        for o in range(6):
            pieces.append(jnp.where(turns == o, value, 0.0).astype(jnp.bfloat16))
    outside = dot(table[:, 128:896], jnp.concatenate(pieces, axis=0))
    inside = inner_high + inner_low

    wall = codes < 0
    normal = [
        flat_row([normals[x, f : f + 1, :] for f in range(4)]) for x in range(3)
    ]
    weight = 0.5 * flat_row([face_scale[f : f + 1, :] * growth for f in range(4)])
    press = jnp.where(wall, 0.0, inside[0:16] - outside[0:16])
    normal_in = None
    for x in range(3):
        term = normal[x] * inside[16 * (x + 1) : 16 * (x + 2)]
        normal_in = term if normal_in is None else normal_in + term
    normal_jump = None
    for x in range(3):
        rows = slice(16 * (x + 1), 16 * (x + 2))
        jump = jnp.where(wall, 2.0 * normal[x] * normal_in, inside[rows] - outside[rows])
        term = normal[x] * jump
        normal_jump = term if normal_jump is None else normal_jump + term
    flux_press = weight * (normal_jump - press)
    fluxes = [flux_press] + [-normal[x] * flux_press for x in range(3)]
    flux = jnp.concatenate(
        [
            jnp.concatenate(
                [flux_c[:, f * elements : (f + 1) * elements] for f in range(4)], axis=0
            )
            for flux_c in fluxes
        ],
        axis=1,
    )
    lifted = dot3(lift_parts, split(flux))
    squares = None
    changes = []
    for c in range(4):
        lift_c = lifted[0:VOLUME_NODES, c * elements : (c + 1) * elements]
        change = base[c, 0:VOLUME_NODES, :] + lift_c
        stored = RUNGE_CARRY * read(store, c) + TIME_STEP * change
        changes.append(change)
        moved = field(c) + RUNGE_ADVANCE * stored
        squares = moved * moved if squares is None else squares + moved * moved
    weighted = absorb * jnp.sum(squares, axis=0, keepdims=True)
    partial = weighted[:, 0:128]
    for at in range(128, elements, 128):
        partial = partial + weighted[:, at : at + 128]
    energy_row[...] = partial

    def write_changes():
        for c in range(4):
            write(change_out, c, TIME_STEP * changes[c])

    def spread_rows(source_row, landing, sent, got, mine, peers, after_sends=lambda: None):
        def copy(peer, device, slot):
            return pltpu.make_async_remote_copy(
                src_ref=source_row,
                dst_ref=landing.at[slot],
                send_sem=sent.at[peer],
                recv_sem=got.at[slot],
                device_id=device,
                device_id_type=MESH,
            )

        for peer, device in peers:
            copy(peer, device, mine).start()
        landing[mine] = source_row[...]
        after_sends()
        for peer, device in peers:
            copy(peer, device, peer).wait_recv()
        for peer, device in peers:
            copy(peer, device, mine).wait_send()
        return jnp.sum(landing[...], axis=0)

    if direct:
        everyone = [
            (grp_peer(kg) * n_sub + sub_peer(ks), (grp_peer(kg), sub_peer(ks)))
            for kg in range(n_grp)
            for ks in range(n_sub)
            if (kg, ks) != (0, 0)
        ]
        total = spread_rows(energy_row, energy_a, esend_a, erecv_a, g * n_sub + s, everyone, write_changes)
    else:
        row_peers = [(sub_peer(k), (g, sub_peer(k))) for k in range(1, n_sub)]
        energy_mid[...] = spread_rows(
            energy_row, energy_a, esend_a, erecv_a, s, row_peers, write_changes
        )
        column_peers = [(grp_peer(k), (grp_peer(k), s)) for k in range(1, n_grp)]
        total = spread_rows(energy_mid, energy_b, esend_b, erecv_b, g, column_peers)
    energy_out[...] = total

    each_sub(sub_copy, lambda copy: copy.wait_send())

    @pl.when(g > 0)
    def _():
        grp_copy(False).wait_send()

    @pl.when(g < n_grp - 1)
    def _():
        grp_copy(True).wait_send()


def finish(divisor, fields, store, stepped, energy, fields_next, store_next, energy_mean):
    energy_mean[...] = jnp.sum(energy[...], axis=1, keepdims=True) / divisor
    moved = RUNGE_CARRY * store[...] + stepped[...]
    store_next[...] = moved
    fields_next[...] = fields[...] + RUNGE_ADVANCE * moved


def local(
    fields,
    section_store,
    metric_terms,
    normals,
    face_scale,
    damping,
    absorb_mask,
    refine_level,
    face_source,
    orientation,
    derivative,
    lift_matrix,
):
    elements = fields.shape[2]
    n_grp, n_sub = lax.axis_size("grp"), lax.axis_size("sub")
    direct = n_grp * n_sub <= 64
    n_blocks = n_sub + 2
    half = elements // 16
    slots_a = n_grp * n_sub if direct else n_sub
    row = lambda value: value.reshape(1, elements)
    vmem = pl.BlockSpec(memory_space=pltpu.VMEM)
    f32 = jnp.float32
    tiles = elements // 128

    def to_rows(value):
        value = value.transpose(1, 0, 2).reshape(VOLUME_NODES, 4, tiles, 128)
        return value.transpose(0, 2, 1, 3).reshape(VOLUME_NODES * tiles * 4, 128)

    def from_rows(value):
        value = value.reshape(VOLUME_NODES, tiles, 4, 128).transpose(0, 2, 1, 3)
        return value.reshape(VOLUME_NODES, 4, elements).transpose(1, 0, 2)

    flat = (VOLUME_NODES * tiles * 4, 128)
    arguments = (
        to_rows(fields),
        to_rows(section_store),
        metric_terms,
        normals.transpose(1, 0, 2),
        face_scale,
        row(damping),
        row(absorb_mask),
        row(refine_level),
        face_source,
        orientation,
        derivative,
        lift_matrix,
        constant_table(),
    )
    held_fields, held_store, stepped, energy = pl.pallas_call(
        functools.partial(kernel, n_grp, n_sub, direct),
        out_shape=(
            pltpu.VMEM(flat, f32),
            pltpu.VMEM(flat, f32),
            pltpu.VMEM(flat, f32),
            pltpu.VMEM((1, 128), f32),
        ),
        in_specs=[pl.BlockSpec(memory_space=pl.ANY)] * OPERANDS,
        out_specs=(vmem, vmem, vmem, vmem),
        scratch_shapes=[pltpu.VMEM(value.shape, value.dtype) for value in arguments[2:]]
        + [
            pltpu.VMEM((NODE_PAD, 4 * elements), f32),
            pltpu.VMEM((3 * SLOPE_PAD, NODE_PAD), f32),
            pltpu.VMEM((SLOPE_PAD, ROWS), f32),
            pltpu.VMEM((n_blocks, half, 2 * ROWS), f32),
            pltpu.VMEM((n_blocks, half, 2 * ROWS), f32),
            pltpu.VMEM((4, SLOPE_PAD, elements), f32),
            pltpu.VMEM((1, 128), f32),
            pltpu.VMEM((1, 128), f32),
            pltpu.VMEM((slots_a, 1, 128), f32),
            pltpu.VMEM((n_grp, 1, 128), f32),
            pltpu.SemaphoreType.DMA((n_blocks,)),
            pltpu.SemaphoreType.DMA((n_blocks,)),
            pltpu.SemaphoreType.DMA((slots_a,)),
            pltpu.SemaphoreType.DMA((slots_a,)),
            pltpu.SemaphoreType.DMA((n_grp,)),
            pltpu.SemaphoreType.DMA((n_grp,)),
            pltpu.SemaphoreType.DMA((OPERANDS,)),
        ],
        compiler_params=pltpu.CompilerParams(collective_id=0, has_side_effects=True),
        name="section",
    )(*arguments)
    held = [
        pltpu.with_memory_space_constraint(value, pltpu.VMEM)
        for value in (held_fields, held_store, stepped, energy)
    ]
    fields_next, store_next, energy = pl.pallas_call(
        functools.partial(finish, elements * n_grp * n_sub * VOLUME_NODES),
        out_shape=(
            jax.ShapeDtypeStruct(flat, f32),
            jax.ShapeDtypeStruct(flat, f32),
            jax.ShapeDtypeStruct((1, 1), f32),
        ),
        in_specs=[vmem] * 4,
        out_specs=(vmem, vmem, vmem),
        name="finish",
    )(*held)
    return from_rows(fields_next), from_rows(store_next), energy.reshape(())


def solution(mesh):
    along = ("grp", "sub")
    placed = (
        P(None, None, along),
        P(None, None, along),
        P(None, along),
        P(None, None, along),
        P(None, along),
        P(along),
        P(along),
        P(along),
        P(None, along),
        P(None, along),
        P(),
        P(),
    )
    return jax.shard_map(
        local,
        mesh=mesh,
        in_specs=placed,
        out_specs=(P(None, None, along), P(None, None, along), P()),
        check_vma=False,
    )
```

```python
import functools

import jax
import jax.numpy as jnp
import numpy as np
from jax import lax
from jax.experimental import pallas as pl
from jax.experimental.pallas import tpu as pltpu
from jax.sharding import PartitionSpec as P

VOLUME_NODES = 35
FACE_NODES = 15
NODE_PAD = 48
SLOPE_PAD = 40
ROWS = 64
TURN_COLS = 768

RUNGE_CARRY = -567301805773.0 / 1357537059087.0
RUNGE_ADVANCE = 5161836677717.0 / 13612068292357.0
TIME_STEP = 0.02
OPERANDS = 14
MESH = pl.DeviceIdType.MESH


def node_tables():
    volume_list = [
        (a, b, c, 4 - a - b - c) for a in range(5) for b in range(5 - a) for c in range(5 - a - b)
    ]
    triples = [(a, b, 4 - a - b) for a in range(5) for b in range(5 - a)]
    face_index = np.zeros((4, 15), np.int32)
    for facet in range(4):
        others = [corner for corner in range(4) if corner != facet]
        for node_pos in range(15):
            corners = [0, 0, 0, 0]
            for place_pos in range(3):
                corners[others[place_pos]] = triples[node_pos][place_pos]
            face_index[facet, node_pos] = volume_list.index(tuple(corners))
    vertex_orders = [(0, 1, 2), (1, 2, 0), (2, 0, 1), (0, 2, 1), (2, 1, 0), (1, 0, 2)]
    turn_index = np.zeros((6, 15), np.int32)
    for option in range(6):
        q = vertex_orders[option]
        for node_pos in range(15):
            t = triples[node_pos]
            turn_index[option, node_pos] = triples.index((t[q[0]], t[q[1]], t[q[2]]))
    return face_index, turn_index


def constant_tables():
    face_index, turn_index = node_tables()
    pick = np.zeros((ROWS, 128), np.float32)
    turn = np.zeros((ROWS, TURN_COLS), np.float32)
    spread = np.zeros((ROWS, 128 + 24 * 16), np.float32)
    for f in range(4):
        for j in range(15):
            pick[f * 16 + j, face_index[f, j]] = 1.0
            spread[f * 15 + j, f * 16 + j] = 1.0
            for o in range(6):
                spread[f * 15 + j, 128 + (f * 6 + o) * 16 + turn_index[o, j]] = 1.0
    for part in range(2):
        for o in range(6):
            for c in range(4):
                for j in range(15):
                    col = part * 384 + o * 64 + c * 16 + turn_index[o, j]
                    turn[c * 16 + j, col] = 1.0
    later = np.concatenate([turn, spread], axis=1)
    return jnp.asarray(pick, jnp.bfloat16), jnp.asarray(later, jnp.bfloat16)


def split(value):
    high = value.astype(jnp.bfloat16)
    low = (value - high.astype(jnp.float32)).astype(jnp.bfloat16)
    return high, low


def dot(left, right):
    return jnp.dot(left, right, preferred_element_type=jnp.float32)


def dot3(left, right):
    (lh, ll), (rh, rl) = left, right
    return dot(lh, rh) + (dot(lh, rl) + dot(ll, rh))


def flat_row(ref_rows):
    return jnp.concatenate(ref_rows, axis=1)


def split3(value):
    high, rest = split(value)
    low = value - high.astype(jnp.float32) - rest.astype(jnp.float32)
    return high, rest, low.astype(jnp.bfloat16)


def kernel(
    n_grp,
    n_sub,
    direct,
    *refs,
):
    operands, rest = refs[:OPERANDS], refs[OPERANDS:]
    results, rest = rest[:3], rest[3:]
    copies, rest = rest[:OPERANDS], rest[OPERANDS:]
    body(n_grp, n_sub, direct, operands, copies, *results, *rest)


def body(
    n_grp,
    n_sub,
    direct,
    operands,
    copies,
    fields_out,
    store_out,
    energy_out,
    fpad,
    dpad,
    lpad,
    outbox,
    inbox,
    moved,
    stored,
    energy_row,
    energy_mid,
    energy_a,
    energy_b,
    trace_sem,
    energy_sem,
    load_sem,
):
    (
        fields,
        store,
        metric,
        normals,
        face_scale,
        damping,
        mask,
        level,
        source,
        orient,
        derivative,
        lift,
        pick_table,
        table,
    ) = copies
    loads = [
        pltpu.make_async_copy(operands[i], copies[i], load_sem.at[i]) for i in range(OPERANDS)
    ]
    early = (0, 8, 12)
    elements = face_scale.shape[1]
    tiles = elements // 128
    faces = 4 * elements
    half = elements // 16
    n_blocks = n_sub + 2

    def node_rows(c, t):
        return pl.ds(t * 4 + c, VOLUME_NODES, stride=4 * tiles)

    def read(ref, c):
        return jnp.concatenate([ref[node_rows(c, t), :] for t in range(tiles)], axis=1)

    def write(ref, c, value):
        for t in range(tiles):
            ref[node_rows(c, t), :] = value[:, t * 128 : (t + 1) * 128]

    g = lax.axis_index("grp")
    s = lax.axis_index("sub")

    def sub_peer(k):
        return lax.rem(s + k, n_sub)

    def grp_peer(k):
        return lax.rem(g + k, n_grp)

    inbox[...] = jnp.zeros_like(inbox)
    for i in early:
        loads[i].start()
    for i in range(OPERANDS):
        if i not in early:
            loads[i].start()
    barrier = pltpu.get_barrier_semaphore()
    for k in range(1, n_sub):
        pl.semaphore_signal(barrier, inc=1, device_id=(g, sub_peer(k)), device_id_type=MESH)
    for k in range(1, n_grp):
        pl.semaphore_signal(barrier, inc=1, device_id=(grp_peer(k), s), device_id_type=MESH)
    greeted = n_sub + n_grp - 2
    for i in early:
        loads[i].wait()

    fpad[VOLUME_NODES:, :] = jnp.zeros((NODE_PAD - VOLUME_NODES, faces), jnp.float32)
    for c in range(4):
        fpad[0:VOLUME_NODES, c * elements : (c + 1) * elements] = read(fields, c)
    field_parts = split(fpad[...])
    pick = pick_table[:, 0:NODE_PAD]

    def by_face(value):
        return jnp.concatenate(
            [
                jnp.concatenate(
                    [
                        value[f * 16 : (f + 1) * 16, c * elements : (c + 1) * elements]
                        for c in range(4)
                    ],
                    axis=0,
                )
                for f in range(4)
            ],
            axis=1,
        )

    inner_high = by_face(dot(pick, field_parts[0]))
    inner_low = by_face(dot(pick, field_parts[1]))
    codes = flat_row([source[f : f + 1, :] for f in range(4)])
    high_b = inner_high.astype(jnp.bfloat16)
    low_b = inner_low.astype(jnp.bfloat16)

    def slots_hot(part):
        row = lax.broadcasted_iota(jnp.int32, (n_blocks * half, faces), 0)
        slot = (row // half) * (2 * half) + part * half + row % half
        return jnp.where(slot == codes - faces, 1.0, 0.0).astype(jnp.bfloat16)

    hot = [slots_hot(0), slots_hot(1)]
    nothing = jnp.zeros_like(high_b)
    packed = None
    for part in range(2):
        for value in (high_b, low_b):
            weights = jnp.concatenate([value, nothing] if part == 0 else [nothing, value], axis=0)
            term = lax.dot_general(
                hot[part], weights, (((1,), (1,)), ((), ())), preferred_element_type=jnp.float32
            )
            packed = term if packed is None else packed + term
    outbox[...] = packed

    pl.semaphore_wait(barrier, greeted)

    def block(ref, at):
        return ref.at[pl.ds(pl.multiple_of(at * half, half), half)]

    def trace_copy(source_block, landing_block, device):
        return pltpu.make_async_remote_copy(
            src_ref=block(outbox, source_block),
            dst_ref=block(inbox, landing_block),
            send_sem=trace_sem.at[0],
            recv_sem=trace_sem.at[1],
            device_id=device,
            device_id_type=MESH,
        )

    def trace_total(blocks):
        return pltpu.make_async_remote_copy(
            src_ref=outbox.at[pl.ds(0, blocks * half)],
            dst_ref=inbox.at[pl.ds(0, blocks * half)],
            send_sem=trace_sem.at[0],
            recv_sem=trace_sem.at[1],
            device_id=(g, sub_peer(1)),
            device_id_type=MESH,
        )

    inner = jnp.logical_and(g > 0, g < n_grp - 1)

    def each_total(act):
        @pl.when(inner)
        def _():
            act(trace_total(n_sub + 1))

        @pl.when(jnp.logical_not(inner))
        def _():
            act(trace_total(n_sub))

    for k in range(1, n_sub):
        trace_copy(sub_peer(k), s, (g, sub_peer(k))).start()

    @pl.when(g > 0)
    def _():
        trace_copy(n_sub, n_sub + 1, (jnp.maximum(g - 1, 0), s)).start()

    @pl.when(g < n_grp - 1)
    def _():
        trace_copy(n_sub + 1, n_sub, (jnp.minimum(g + 1, n_grp - 1), s)).start()

    for i in range(OPERANDS):
        if i not in early:
            loads[i].wait()
    growth = jnp.exp2(level[...].astype(jnp.float32))
    absorb = damping[...] * mask[...].astype(jnp.float32)
    dpad[...] = jnp.zeros_like(dpad)
    for d in range(3):
        dpad[d * SLOPE_PAD : d * SLOPE_PAD + VOLUME_NODES, 0:VOLUME_NODES] = derivative[d]
    slopes = dot3(split(dpad[...]), field_parts)

    def slope(d, c):
        return slopes[
            d * SLOPE_PAD : (d + 1) * SLOPE_PAD, c * elements : (c + 1) * elements
        ]

    def field(c):
        return fpad[0:VOLUME_NODES, c * elements : (c + 1) * elements]

    lpad[...] = jnp.zeros_like(lpad)
    lpad[0:VOLUME_NODES, 0:60] = lift[...]
    spread = table[:, TURN_COLS : TURN_COLS + ROWS]
    turned_spread = table[:, TURN_COLS + 128 : TURN_COLS + 128 + 24 * 16]
    lift_split = split(lpad[...])
    lift_parts = tuple(dot(part, spread).astype(jnp.bfloat16) for part in lift_split)
    turned_lift = tuple(dot(part, turned_spread).astype(jnp.bfloat16) for part in lift_split)

    stacked = jnp.concatenate([high_b, low_b], axis=0)
    gathered = None
    for f in range(4):
        row = lax.broadcasted_iota(jnp.int32, (elements, faces), 0) + f * elements
        chosen = jnp.where(row == codes, 1.0, 0.0).astype(jnp.bfloat16)
        term = dot(stacked[:, f * elements : (f + 1) * elements], chosen)
        gathered = term if gathered is None else gathered + term

    turns = flat_row([orient[f : f + 1, :] for f in range(4)])
    pieces = []
    for part in range(2):
        value = gathered[part * ROWS : (part + 1) * ROWS]
        for o in range(6):
            pieces.append(jnp.where(turns == o, value, 0.0).astype(jnp.bfloat16))
    outside = dot(table[:, 0:TURN_COLS], jnp.concatenate(pieces, axis=0))
    inside = inner_high + inner_low

    wall = codes < 0
    normal = [
        flat_row([normals[x, f : f + 1, :] for f in range(4)]) for x in range(3)
    ]
    weight = 0.5 * flat_row([face_scale[f : f + 1, :] * growth for f in range(4)])
    press = jnp.where(wall, 0.0, inside[0:16] - outside[0:16])
    normal_in = None
    for x in range(3):
        term = normal[x] * inside[16 * (x + 1) : 16 * (x + 2)]
        normal_in = term if normal_in is None else normal_in + term
    normal_jump = None
    for x in range(3):
        rows = slice(16 * (x + 1), 16 * (x + 2))
        jump = jnp.where(wall, 2.0 * normal[x] * normal_in, inside[rows] - outside[rows])
        term = normal[x] * jump
        normal_jump = term if normal_jump is None else normal_jump + term
    flux_press = weight * (normal_jump - press)
    fluxes = [flux_press] + [-normal[x] * flux_press for x in range(3)]
    flux = jnp.concatenate(
        [
            jnp.concatenate(
                [flux_c[:, f * elements : (f + 1) * elements] for f in range(4)], axis=0
            )
            for flux_c in fluxes
        ],
        axis=1,
    )
    lifted = dot3(lift_parts, split(flux))
    scaled = metric[...] * growth
    for c in range(4):
        total = None
        for x in range(3) if c == 0 else (c - 1,):
            for y in range(3):
                term = scaled[3 * x + y : 3 * x + y + 1, :] * slope(y, x + 1 if c == 0 else 0)
                total = term if total is None else total + term
        lift_c = lifted[:, c * elements : (c + 1) * elements]
        change = lift_c - total - absorb * fpad[0:SLOPE_PAD, c * elements : (c + 1) * elements]
        stepped = TIME_STEP * change[0:VOLUME_NODES] + RUNGE_CARRY * read(store, c)
        stored[c, 0:VOLUME_NODES, :] = stepped
        moved[c, 0:VOLUME_NODES, :] = field(c) + RUNGE_ADVANCE * stepped
        for ref in (stored, moved):
            ref[c, VOLUME_NODES:, :] = jnp.zeros((SLOPE_PAD - VOLUME_NODES, elements), jnp.float32)

    face_row = lax.broadcasted_iota(jnp.int32, (1, faces), 1) // elements
    kinds = (face_row * 6 + turns).astype(jnp.bfloat16)
    meta_rows = []
    for value in normal + [TIME_STEP * weight]:
        meta_rows.extend(split3(value))
    meta = jnp.concatenate(
        [row.astype(jnp.float32) for row in meta_rows]
        + [kinds.astype(jnp.float32)]
        + [jnp.zeros((3, faces), jnp.float32)],
        axis=0,
    ).astype(jnp.bfloat16)
    slot_normal, slot_weight, slot_kind, slot_element = [], [], [], []
    for part in range(2):
        found = lax.dot_general(
            meta, hot[part], (((1,), (1,)), ((), ())), preferred_element_type=jnp.float32
        )
        rows = [
            found[3 * i : 3 * i + 1] + (found[3 * i + 1 : 3 * i + 2] + found[3 * i + 2 : 3 * i + 3])
            for i in range(4)
        ]
        slot_normal.append(rows[:3])
        slot_weight.append(rows[3])
        slot_kind.append(found[12:13].astype(jnp.int32))
        at_element = hot[part][:, 0:elements]
        for f in range(1, 4):
            at_element = at_element + hot[part][:, f * elements : (f + 1) * elements]
        slot_element.append(at_element)

    each_total(lambda copy: copy.wait_recv())

    arrived = inbox[...].T
    landed = None
    for part in range(2):
        value = arrived[part * ROWS : (part + 1) * ROWS]
        outer = value[0:16]
        for x in range(3):
            outer = outer - slot_normal[part][x] * value[16 * (x + 1) : 16 * (x + 2)]
        outer_parts = split(slot_weight[part] * outer)
        spread_parts = [
            jnp.concatenate(
                [
                    jnp.where(slot_kind[part] == kind, piece, jnp.zeros_like(piece))
                    for kind in range(24)
                ],
                axis=0,
            )
            for piece in outer_parts
        ]
        press_lift = dot3(turned_lift, spread_parts)
        slot_lift = jnp.concatenate(
            [press_lift] + [-slot_normal[part][x] * press_lift for x in range(3)], axis=0
        )
        slot_parts = jnp.concatenate(split(slot_lift), axis=0)
        term = dot(slot_parts, slot_element[part])
        landed = term if landed is None else landed + term
    remote = landed[0 : 4 * SLOPE_PAD] + landed[4 * SLOPE_PAD :]
    squares = None
    for c in range(4):
        remote_c = remote[c * SLOPE_PAD : (c + 1) * SLOPE_PAD]
        moved_c = moved[c] + RUNGE_ADVANCE * remote_c
        moved[c] = moved_c
        stored[c] = stored[c] + remote_c
        squares = moved_c * moved_c if squares is None else squares + moved_c * moved_c
    weighted = absorb * jnp.sum(squares, axis=0, keepdims=True)
    partial = weighted[:, 0:128]
    for at in range(128, elements, 128):
        partial = partial + weighted[:, at : at + 128]
    energy_row[...] = partial

    def write_results():
        for c in range(4):
            write(fields_out, c, moved[c, 0:VOLUME_NODES, :])
            write(store_out, c, stored[c, 0:VOLUME_NODES, :])

    def spread_rows(source_row, landing, stage, mine, peers, after_sends=lambda: None):
        def copy(source, target, device):
            return pltpu.make_async_remote_copy(
                src_ref=source,
                dst_ref=target,
                send_sem=energy_sem.at[2 * stage],
                recv_sem=energy_sem.at[2 * stage + 1],
                device_id=device,
                device_id_type=MESH,
            )

        for device in peers:
            copy(source_row, landing.at[mine], device).start()
        landing[mine] = source_row[...]
        after_sends()
        others = landing.at[pl.ds(0, len(peers))]
        total = copy(others, others, peers[0])
        total.wait_recv()
        total.wait_send()
        return jnp.sum(landing[...], axis=0)

    if direct:
        everyone = [
            (grp_peer(kg), sub_peer(ks))
            for kg in range(n_grp)
            for ks in range(n_sub)
            if (kg, ks) != (0, 0)
        ]
        total = spread_rows(energy_row, energy_a, 0, g * n_sub + s, everyone, write_results)
    else:
        row_peers = [(g, sub_peer(k)) for k in range(1, n_sub)]
        energy_mid[...] = spread_rows(energy_row, energy_a, 0, s, row_peers, write_results)
        column_peers = [(grp_peer(k), s) for k in range(1, n_grp)]
        total = spread_rows(energy_mid, energy_b, 1, g, column_peers)
    energy_out[...] = total
    each_total(lambda copy: copy.wait_send())


def finish(divisor, fields, store, energy, fields_next, store_next, energy_mean, mean, sem):
    copies = [
        pltpu.make_async_copy(source, target, sem.at[i])
        for i, (source, target) in enumerate(
            [(fields, fields_next), (store, store_next), (mean, energy_mean)]
        )
    ]
    copies[0].start()
    copies[1].start()
    mean[...] = jnp.sum(energy[...], axis=1, keepdims=True) / divisor
    copies[2].start()
    for copy in copies:
        copy.wait()


def local(
    fields,
    section_store,
    metric_terms,
    normals,
    face_scale,
    damping,
    absorb_mask,
    refine_level,
    face_source,
    orientation,
    derivative,
    lift_matrix,
):
    elements = fields.shape[2]
    n_grp, n_sub = lax.axis_size("grp"), lax.axis_size("sub")
    direct = n_grp * n_sub <= 64
    n_blocks = n_sub + 2
    half = elements // 16
    slots_a = n_grp * n_sub if direct else n_sub
    row = lambda value: value.reshape(1, elements)
    vmem = pl.BlockSpec(memory_space=pltpu.VMEM)
    anywhere = pl.BlockSpec(memory_space=pl.ANY)
    f32 = jnp.float32
    tiles = elements // 128

    def to_rows(value):
        value = value.transpose(1, 0, 2).reshape(VOLUME_NODES, 4, tiles, 128)
        return value.transpose(0, 2, 1, 3).reshape(VOLUME_NODES * tiles * 4, 128)

    def from_rows(value):
        value = value.reshape(VOLUME_NODES, tiles, 4, 128).transpose(0, 2, 1, 3)
        return value.reshape(VOLUME_NODES, 4, elements).transpose(1, 0, 2)

    flat = (VOLUME_NODES * tiles * 4, 128)
    arguments = (
        to_rows(fields),
        to_rows(section_store),
        metric_terms,
        normals.transpose(1, 0, 2),
        face_scale,
        row(damping),
        row(absorb_mask),
        row(refine_level),
        face_source,
        orientation,
        derivative,
        lift_matrix,
        *constant_tables(),
    )
    held = pl.pallas_call(
        functools.partial(kernel, n_grp, n_sub, direct),
        out_shape=(pltpu.VMEM(flat, f32), pltpu.VMEM(flat, f32), pltpu.VMEM((1, 128), f32)),
        in_specs=[anywhere] * OPERANDS,
        out_specs=(vmem,) * 3,
        scratch_shapes=[pltpu.VMEM(value.shape, value.dtype) for value in arguments]
        + [
            pltpu.VMEM((NODE_PAD, 4 * elements), f32),
            pltpu.VMEM((3 * SLOPE_PAD, NODE_PAD), f32),
            pltpu.VMEM((SLOPE_PAD, ROWS), f32),
            pltpu.VMEM((n_blocks * half, 2 * ROWS), f32),
            pltpu.VMEM((n_blocks * half, 2 * ROWS), f32),
            pltpu.VMEM((4, SLOPE_PAD, elements), f32),
            pltpu.VMEM((4, SLOPE_PAD, elements), f32),
            pltpu.VMEM((1, 128), f32),
            pltpu.VMEM((1, 128), f32),
            pltpu.VMEM((slots_a, 1, 128), f32),
            pltpu.VMEM((n_grp, 1, 128), f32),
            pltpu.SemaphoreType.DMA((2,)),
            pltpu.SemaphoreType.DMA((2 if direct else 4,)),
            pltpu.SemaphoreType.DMA((OPERANDS,)),
        ],
        compiler_params=pltpu.CompilerParams(collective_id=0, has_side_effects=True),
        name="section",
    )(*arguments)
    held = [pltpu.with_memory_space_constraint(value, pltpu.VMEM) for value in held]
    fields_next, store_next, energy = pl.pallas_call(
        functools.partial(finish, elements * n_grp * n_sub * VOLUME_NODES),
        out_shape=(
            jax.ShapeDtypeStruct(flat, f32),
            jax.ShapeDtypeStruct(flat, f32),
            jax.ShapeDtypeStruct((1, 1), f32),
        ),
        in_specs=[vmem] * 3,
        out_specs=(anywhere,) * 3,
        scratch_shapes=[pltpu.VMEM((1, 1), f32), pltpu.SemaphoreType.DMA((3,))],
        name="finish",
    )(*held)
    return from_rows(fields_next), from_rows(store_next), energy.reshape(())


def solution(mesh):
    along = ("grp", "sub")
    placed = (
        P(None, None, along),
        P(None, None, along),
        P(None, along),
        P(None, None, along),
        P(None, along),
        P(along),
        P(along),
        P(along),
        P(None, along),
        P(None, along),
        P(),
        P(),
    )
    return jax.shard_map(
        local,
        mesh=mesh,
        in_specs=placed,
        out_specs=(P(None, None, along), P(None, None, along), P()),
        check_vma=False,
    )
```

```python
import functools

import jax
import jax.numpy as jnp
import numpy as np
from jax import lax
from jax.experimental import pallas as pl
from jax.experimental.pallas import tpu as pltpu
from jax.sharding import PartitionSpec as P

VOLUME_NODES = 35
FACE_NODES = 15
NODE_PAD = 48
SLOPE_PAD = 40
ROWS = 64
TURN_COLS = 768

RUNGE_CARRY = -567301805773.0 / 1357537059087.0
RUNGE_ADVANCE = 5161836677717.0 / 13612068292357.0
TIME_STEP = 0.02
OPERANDS = 14
MESH = pl.DeviceIdType.MESH


def node_tables():
    volume_list = [
        (a, b, c, 4 - a - b - c) for a in range(5) for b in range(5 - a) for c in range(5 - a - b)
    ]
    triples = [(a, b, 4 - a - b) for a in range(5) for b in range(5 - a)]
    face_index = np.zeros((4, 15), np.int32)
    for facet in range(4):
        others = [corner for corner in range(4) if corner != facet]
        for node_pos in range(15):
            corners = [0, 0, 0, 0]
            for place_pos in range(3):
                corners[others[place_pos]] = triples[node_pos][place_pos]
            face_index[facet, node_pos] = volume_list.index(tuple(corners))
    vertex_orders = [(0, 1, 2), (1, 2, 0), (2, 0, 1), (0, 2, 1), (2, 1, 0), (1, 0, 2)]
    turn_index = np.zeros((6, 15), np.int32)
    for option in range(6):
        q = vertex_orders[option]
        for node_pos in range(15):
            t = triples[node_pos]
            turn_index[option, node_pos] = triples.index((t[q[0]], t[q[1]], t[q[2]]))
    return face_index, turn_index


def constant_tables():
    face_index, turn_index = node_tables()
    pick = np.zeros((ROWS, 128), np.float32)
    turn = np.zeros((ROWS, TURN_COLS), np.float32)
    spread = np.zeros((ROWS, 128 + 24 * 16), np.float32)
    for f in range(4):
        for j in range(15):
            pick[f * 16 + j, face_index[f, j]] = 1.0
            spread[f * 15 + j, f * 16 + j] = 1.0
            for o in range(6):
                spread[f * 15 + j, 128 + (f * 6 + o) * 16 + turn_index[o, j]] = 1.0
    for part in range(2):
        for o in range(6):
            for c in range(4):
                for j in range(15):
                    col = part * 384 + o * 64 + c * 16 + turn_index[o, j]
                    turn[c * 16 + j, col] = 1.0
    later = np.concatenate([turn, spread], axis=1)
    return jnp.asarray(pick, jnp.bfloat16), jnp.asarray(later, jnp.bfloat16)


def split(value):
    high = value.astype(jnp.bfloat16)
    low = (value - high.astype(jnp.float32)).astype(jnp.bfloat16)
    return high, low


def dot(left, right):
    return jnp.dot(left, right, preferred_element_type=jnp.float32)


def dot3(left, right):
    (lh, ll), (rh, rl) = left, right
    return dot(lh, rh) + (dot(lh, rl) + dot(ll, rh))


def flat_row(ref_rows):
    return jnp.concatenate(ref_rows, axis=1)


def split3(value):
    high, rest = split(value)
    low = value - high.astype(jnp.float32) - rest.astype(jnp.float32)
    return high, rest, low.astype(jnp.bfloat16)


def kernel(
    n_grp,
    n_sub,
    direct,
    *refs,
):
    operands, rest = refs[:OPERANDS], refs[OPERANDS:]
    results, rest = rest[:3], rest[3:]
    copies, rest = rest[:OPERANDS], rest[OPERANDS:]
    body(n_grp, n_sub, direct, operands, copies, *results, *rest)


def body(
    n_grp,
    n_sub,
    direct,
    operands,
    copies,
    fields_out,
    store_out,
    energy_out,
    fpad,
    dpad,
    lpad,
    outbox,
    inbox,
    moved,
    stored,
    kind_mask,
    energy_row,
    energy_mid,
    energy_a,
    energy_b,
    trace_sem,
    energy_sem,
    load_sem,
):
    (
        fields,
        store,
        metric,
        normals,
        face_scale,
        damping,
        mask,
        level,
        source,
        orient,
        derivative,
        lift,
        pick_table,
        table,
    ) = copies
    loads = [
        pltpu.make_async_copy(operands[i], copies[i], load_sem.at[i]) for i in range(OPERANDS)
    ]
    early = (0, 8, 12)
    elements = face_scale.shape[1]
    tiles = elements // 128
    faces = 4 * elements
    half = elements // 16
    n_blocks = n_sub + 2

    def node_rows(c, t):
        return pl.ds(t * 4 + c, VOLUME_NODES, stride=4 * tiles)

    def read(ref, c):
        return jnp.concatenate([ref[node_rows(c, t), :] for t in range(tiles)], axis=1)

    def write(ref, c, value):
        for t in range(tiles):
            ref[node_rows(c, t), :] = value[:, t * 128 : (t + 1) * 128]

    g = lax.axis_index("grp")
    s = lax.axis_index("sub")

    def sub_peer(k):
        return lax.rem(s + k, n_sub)

    def grp_peer(k):
        return lax.rem(g + k, n_grp)

    inbox[...] = jnp.zeros_like(inbox)
    barrier = pltpu.get_barrier_semaphore()
    for k in range(1, n_sub):
        pl.semaphore_signal(barrier, inc=1, device_id=(g, sub_peer(k)), device_id_type=MESH)
    for k in range(1, n_grp):
        pl.semaphore_signal(barrier, inc=1, device_id=(grp_peer(k), s), device_id_type=MESH)
    for i in early:
        loads[i].start()
    for i in range(OPERANDS):
        if i not in early:
            loads[i].start()
    greeted = n_sub + n_grp - 2
    for i in early:
        loads[i].wait()

    fpad[VOLUME_NODES:, :] = jnp.zeros((NODE_PAD - VOLUME_NODES, faces), jnp.float32)
    for c in range(4):
        fpad[0:VOLUME_NODES, c * elements : (c + 1) * elements] = read(fields, c)
    field_parts = split(fpad[...])
    pick = pick_table[:, 0:NODE_PAD]

    def by_face(value):
        return jnp.concatenate(
            [
                jnp.concatenate(
                    [
                        value[f * 16 : (f + 1) * 16, c * elements : (c + 1) * elements]
                        for c in range(4)
                    ],
                    axis=0,
                )
                for f in range(4)
            ],
            axis=1,
        )

    inner_high = by_face(dot(pick, field_parts[0]))
    inner_low = by_face(dot(pick, field_parts[1]))
    codes = flat_row([source[f : f + 1, :] for f in range(4)])
    high_b = inner_high.astype(jnp.bfloat16)
    low_b = inner_low.astype(jnp.bfloat16)

    def slots_hot(part):
        row = lax.broadcasted_iota(jnp.int32, (n_blocks * half, faces), 0)
        slot = (row // half) * (2 * half) + part * half + row % half
        return jnp.where(slot == codes - faces, 1.0, 0.0).astype(jnp.bfloat16)

    hot = [slots_hot(0), slots_hot(1)]
    nothing = jnp.zeros_like(high_b)
    packed = None
    for part in range(2):
        for value in (high_b, low_b):
            weights = jnp.concatenate([value, nothing] if part == 0 else [nothing, value], axis=0)
            term = lax.dot_general(
                hot[part], weights, (((1,), (1,)), ((), ())), preferred_element_type=jnp.float32
            )
            packed = term if packed is None else packed + term
    outbox[...] = packed

    pl.semaphore_wait(barrier, greeted)

    def block(ref, at):
        return ref.at[pl.ds(pl.multiple_of(at * half, half), half)]

    def trace_copy(source_block, landing_block, device):
        return pltpu.make_async_remote_copy(
            src_ref=block(outbox, source_block),
            dst_ref=block(inbox, landing_block),
            send_sem=trace_sem.at[0],
            recv_sem=trace_sem.at[1],
            device_id=device,
            device_id_type=MESH,
        )

    def trace_total(blocks):
        return pltpu.make_async_remote_copy(
            src_ref=outbox.at[pl.ds(0, blocks * half)],
            dst_ref=inbox.at[pl.ds(0, blocks * half)],
            send_sem=trace_sem.at[0],
            recv_sem=trace_sem.at[1],
            device_id=(g, sub_peer(1)),
            device_id_type=MESH,
        )

    inner = jnp.logical_and(g > 0, g < n_grp - 1)

    def each_total(act):
        @pl.when(inner)
        def _():
            act(trace_total(n_sub + 1))

        @pl.when(jnp.logical_not(inner))
        def _():
            act(trace_total(n_sub))

    for k in range(n_sub - 2, -1, -1):
        peer = jnp.where(k < s, k, k + 1)
        trace_copy(peer, s, (g, peer)).start()

    @pl.when(g > 0)
    def _():
        trace_copy(n_sub, n_sub + 1, (jnp.maximum(g - 1, 0), s)).start()

    @pl.when(g < n_grp - 1)
    def _():
        trace_copy(n_sub + 1, n_sub, (jnp.minimum(g + 1, n_grp - 1), s)).start()

    for i in range(OPERANDS):
        if i not in early:
            loads[i].wait()
    growth = jnp.exp2(level[...].astype(jnp.float32))
    absorb = damping[...] * mask[...].astype(jnp.float32)
    dpad[...] = jnp.zeros_like(dpad)
    for d in range(3):
        dpad[d * SLOPE_PAD : d * SLOPE_PAD + VOLUME_NODES, 0:VOLUME_NODES] = derivative[d]
    slopes = dot3(split(dpad[...]), field_parts)

    def slope(d, c):
        return slopes[
            d * SLOPE_PAD : (d + 1) * SLOPE_PAD, c * elements : (c + 1) * elements
        ]

    def field(c):
        return fpad[0:VOLUME_NODES, c * elements : (c + 1) * elements]

    lpad[...] = jnp.zeros_like(lpad)
    lpad[0:VOLUME_NODES, 0:60] = lift[...]
    spread = table[:, TURN_COLS : TURN_COLS + ROWS]
    turned_spread = table[:, TURN_COLS + 128 : TURN_COLS + 128 + 24 * 16]
    lift_split = split(lpad[...])
    lift_parts = tuple(dot(part, spread).astype(jnp.bfloat16) for part in lift_split)
    turned_lift = tuple(dot(part, turned_spread).astype(jnp.bfloat16) for part in lift_split)

    stacked = jnp.concatenate([high_b, low_b], axis=0)
    gathered = None
    for f in range(4):
        row = lax.broadcasted_iota(jnp.int32, (elements, faces), 0) + f * elements
        chosen = jnp.where(row == codes, 1.0, 0.0).astype(jnp.bfloat16)
        term = dot(stacked[:, f * elements : (f + 1) * elements], chosen)
        gathered = term if gathered is None else gathered + term

    turns = flat_row([orient[f : f + 1, :] for f in range(4)])
    pieces = []
    for part in range(2):
        value = gathered[part * ROWS : (part + 1) * ROWS]
        for o in range(6):
            pieces.append(jnp.where(turns == o, value, 0.0).astype(jnp.bfloat16))
    outside = dot(table[:, 0:TURN_COLS], jnp.concatenate(pieces, axis=0))
    inside = inner_high + inner_low

    wall = codes < 0
    normal = [
        flat_row([normals[x, f : f + 1, :] for f in range(4)]) for x in range(3)
    ]
    weight = 0.5 * flat_row([face_scale[f : f + 1, :] * growth for f in range(4)])
    press = jnp.where(wall, 0.0, inside[0:16] - outside[0:16])
    normal_in = None
    for x in range(3):
        term = normal[x] * inside[16 * (x + 1) : 16 * (x + 2)]
        normal_in = term if normal_in is None else normal_in + term
    normal_jump = None
    for x in range(3):
        rows = slice(16 * (x + 1), 16 * (x + 2))
        jump = jnp.where(wall, 2.0 * normal[x] * normal_in, inside[rows] - outside[rows])
        term = normal[x] * jump
        normal_jump = term if normal_jump is None else normal_jump + term
    flux_press = weight * (normal_jump - press)
    fluxes = [flux_press] + [-normal[x] * flux_press for x in range(3)]
    flux = jnp.concatenate(
        [
            jnp.concatenate(
                [flux_c[:, f * elements : (f + 1) * elements] for f in range(4)], axis=0
            )
            for flux_c in fluxes
        ],
        axis=1,
    )
    lifted = dot3(lift_parts, split(flux))
    scaled = metric[...] * growth
    for c in range(4):
        total = None
        for x in range(3) if c == 0 else (c - 1,):
            for y in range(3):
                term = scaled[3 * x + y : 3 * x + y + 1, :] * slope(y, x + 1 if c == 0 else 0)
                total = term if total is None else total + term
        lift_c = lifted[:, c * elements : (c + 1) * elements]
        change = lift_c - total - absorb * fpad[0:SLOPE_PAD, c * elements : (c + 1) * elements]
        stepped = TIME_STEP * change[0:VOLUME_NODES] + RUNGE_CARRY * read(store, c)
        stored[c, 0:VOLUME_NODES, :] = stepped
        moved[c, 0:VOLUME_NODES, :] = field(c) + RUNGE_ADVANCE * stepped
        for ref in (stored, moved):
            ref[c, VOLUME_NODES:, :] = jnp.zeros((SLOPE_PAD - VOLUME_NODES, elements), jnp.float32)

    face_row = lax.broadcasted_iota(jnp.int32, (1, faces), 1) // elements
    kinds = (face_row * 6 + turns).astype(jnp.bfloat16)
    meta_rows = []
    for value in normal + [TIME_STEP * weight]:
        meta_rows.extend(split3(value))
    meta = jnp.concatenate(
        [row.astype(jnp.float32) for row in meta_rows]
        + [kinds.astype(jnp.float32)]
        + [jnp.zeros((3, faces), jnp.float32)],
        axis=0,
    ).astype(jnp.bfloat16)
    slot_normal, slot_weight, slot_element = [], [], []
    for part in range(2):
        found = lax.dot_general(
            meta, hot[part], (((1,), (1,)), ((), ())), preferred_element_type=jnp.float32
        )
        rows = [
            found[3 * i : 3 * i + 1] + (found[3 * i + 1 : 3 * i + 2] + found[3 * i + 2 : 3 * i + 3])
            for i in range(4)
        ]
        slot_normal.append(rows[:3])
        slot_weight.append(rows[3])
        kind = jnp.broadcast_to(found[12:13], (16, n_blocks * half))
        for at in range(24):
            kind_mask[part, at * 16 : (at + 1) * 16, :] = jnp.where(
                kind == at, 1.0, 0.0
            ).astype(jnp.bfloat16)
        at_element = hot[part][:, 0:elements]
        for f in range(1, 4):
            at_element = at_element + hot[part][:, f * elements : (f + 1) * elements]
        slot_element.append(at_element)

    each_total(lambda copy: copy.wait_recv())

    arrived = inbox[...].T
    landed = None
    for part in range(2):
        value = arrived[part * ROWS : (part + 1) * ROWS]
        outer = value[0:16]
        for x in range(3):
            outer = outer - slot_normal[part][x] * value[16 * (x + 1) : 16 * (x + 2)]
        outer_parts = split(slot_weight[part] * outer)
        spread_parts = [
            jnp.concatenate([piece] * 24, axis=0) * kind_mask[part] for piece in outer_parts
        ]
        press_lift = dot3(turned_lift, spread_parts)
        slot_lift = jnp.concatenate(
            [press_lift] + [-slot_normal[part][x] * press_lift for x in range(3)], axis=0
        )
        slot_parts = jnp.concatenate(split(slot_lift), axis=0)
        term = dot(slot_parts, slot_element[part])
        landed = term if landed is None else landed + term
    remote = landed[0 : 4 * SLOPE_PAD] + landed[4 * SLOPE_PAD :]
    squares = None
    for c in range(4):
        remote_c = remote[c * SLOPE_PAD : (c + 1) * SLOPE_PAD]
        moved_c = moved[c] + RUNGE_ADVANCE * remote_c
        moved[c] = moved_c
        stored[c] = stored[c] + remote_c
        squares = moved_c * moved_c if squares is None else squares + moved_c * moved_c
    weighted = absorb * jnp.sum(squares, axis=0, keepdims=True)
    partial = weighted[:, 0:128]
    for at in range(128, elements, 128):
        partial = partial + weighted[:, at : at + 128]
    energy_row[...] = partial

    def write_results():
        for c in range(4):
            write(fields_out, c, moved[c, 0:VOLUME_NODES, :])
            write(store_out, c, stored[c, 0:VOLUME_NODES, :])

    def spread_rows(source_row, landing, stage, mine, peers, after_sends=lambda: None):
        def copy(source, target, device):
            return pltpu.make_async_remote_copy(
                src_ref=source,
                dst_ref=target,
                send_sem=energy_sem.at[2 * stage],
                recv_sem=energy_sem.at[2 * stage + 1],
                device_id=device,
                device_id_type=MESH,
            )

        for device in peers:

            @pl.when(jnp.logical_or(device[0] != g, device[1] != s))
            def _():
                copy(source_row, landing.at[mine], device).start()

        landing[mine] = source_row[...]
        after_sends()
        others = landing.at[pl.ds(0, len(peers) - 1)]
        total = copy(others, others, (g, sub_peer(1)))
        total.wait_recv()
        total.wait_send()
        return jnp.sum(landing[...], axis=0)

    if direct:
        everyone = [(kg, ks) for ks in range(n_sub) for kg in range(n_grp)]
        total = spread_rows(energy_row, energy_a, 0, g * n_sub + s, everyone, write_results)
    else:
        row_peers = [(g, k) for k in range(n_sub)]
        energy_mid[...] = spread_rows(energy_row, energy_a, 0, s, row_peers, write_results)
        column_peers = [(k, s) for k in range(n_grp)]
        total = spread_rows(energy_mid, energy_b, 1, g, column_peers)
    energy_out[...] = total
    each_total(lambda copy: copy.wait_send())


def finish(divisor, fields, store, energy, fields_next, store_next, energy_mean, mean, sem):
    copies = [
        pltpu.make_async_copy(source, target, sem.at[i])
        for i, (source, target) in enumerate(
            [(fields, fields_next), (store, store_next), (mean, energy_mean)]
        )
    ]
    copies[0].start()
    copies[1].start()
    mean[...] = jnp.sum(energy[...], axis=1, keepdims=True) / divisor
    copies[2].start()
    for copy in copies:
        copy.wait()


def local(
    fields,
    section_store,
    metric_terms,
    normals,
    face_scale,
    damping,
    absorb_mask,
    refine_level,
    face_source,
    orientation,
    derivative,
    lift_matrix,
):
    elements = fields.shape[2]
    n_grp, n_sub = lax.axis_size("grp"), lax.axis_size("sub")
    direct = n_grp * n_sub <= 64
    n_blocks = n_sub + 2
    half = elements // 16
    slots_a = n_grp * n_sub if direct else n_sub
    row = lambda value: value.reshape(1, elements)
    vmem = pl.BlockSpec(memory_space=pltpu.VMEM)
    anywhere = pl.BlockSpec(memory_space=pl.ANY)
    f32 = jnp.float32
    tiles = elements // 128

    def to_rows(value):
        value = value.transpose(1, 0, 2).reshape(VOLUME_NODES, 4, tiles, 128)
        return value.transpose(0, 2, 1, 3).reshape(VOLUME_NODES * tiles * 4, 128)

    def from_rows(value):
        value = value.reshape(VOLUME_NODES, tiles, 4, 128).transpose(0, 2, 1, 3)
        return value.reshape(VOLUME_NODES, 4, elements).transpose(1, 0, 2)

    flat = (VOLUME_NODES * tiles * 4, 128)
    arguments = (
        to_rows(fields),
        to_rows(section_store),
        metric_terms,
        normals.transpose(1, 0, 2),
        face_scale,
        row(damping),
        row(absorb_mask),
        row(refine_level),
        face_source,
        orientation,
        derivative,
        lift_matrix,
        *constant_tables(),
    )
    held = pl.pallas_call(
        functools.partial(kernel, n_grp, n_sub, direct),
        out_shape=(pltpu.VMEM(flat, f32), pltpu.VMEM(flat, f32), pltpu.VMEM((1, 128), f32)),
        in_specs=[anywhere] * OPERANDS,
        out_specs=(vmem,) * 3,
        scratch_shapes=[pltpu.VMEM(value.shape, value.dtype) for value in arguments]
        + [
            pltpu.VMEM((NODE_PAD, 4 * elements), f32),
            pltpu.VMEM((3 * SLOPE_PAD, NODE_PAD), f32),
            pltpu.VMEM((SLOPE_PAD, ROWS), f32),
            pltpu.VMEM((n_blocks * half, 2 * ROWS), f32),
            pltpu.VMEM((n_blocks * half, 2 * ROWS), f32),
            pltpu.VMEM((4, SLOPE_PAD, elements), f32),
            pltpu.VMEM((4, SLOPE_PAD, elements), f32),
            pltpu.VMEM((2, 24 * 16, n_blocks * half), jnp.bfloat16),
            pltpu.VMEM((1, 128), f32),
            pltpu.VMEM((1, 128), f32),
            pltpu.VMEM((slots_a, 1, 128), f32),
            pltpu.VMEM((n_grp, 1, 128), f32),
            pltpu.SemaphoreType.DMA((2,)),
            pltpu.SemaphoreType.DMA((2 if direct else 4,)),
            pltpu.SemaphoreType.DMA((OPERANDS,)),
        ],
        compiler_params=pltpu.CompilerParams(collective_id=0, has_side_effects=True),
        name="section",
    )(*arguments)
    held = [pltpu.with_memory_space_constraint(value, pltpu.VMEM) for value in held]
    fields_next, store_next, energy = pl.pallas_call(
        functools.partial(finish, elements * n_grp * n_sub * VOLUME_NODES),
        out_shape=(
            jax.ShapeDtypeStruct(flat, f32),
            jax.ShapeDtypeStruct(flat, f32),
            jax.ShapeDtypeStruct((1, 1), f32),
        ),
        in_specs=[vmem] * 3,
        out_specs=(anywhere,) * 3,
        scratch_shapes=[pltpu.VMEM((1, 1), f32), pltpu.SemaphoreType.DMA((3,))],
        name="finish",
    )(*held)
    return from_rows(fields_next), from_rows(store_next), energy.reshape(())


def solution(mesh):
    along = ("grp", "sub")
    placed = (
        P(None, None, along),
        P(None, None, along),
        P(None, along),
        P(None, None, along),
        P(None, along),
        P(along),
        P(along),
        P(along),
        P(None, along),
        P(None, along),
        P(),
        P(),
    )
    return jax.shard_map(
        local,
        mesh=mesh,
        in_specs=placed,
        out_specs=(P(None, None, along), P(None, None, along), P()),
        check_vma=False,
    )
```
